512 devices in a mesh: band: 32 (over y, x_hi, core), samp: 16 (over z, x_lo).
Axes of the slice: x: 4 (x_hi: 2, x_lo: 2; x = x_hi * 2 + x_lo), y: 8, z: 8, core: 2. Of those that a mesh axis runs over, the one named last changes fastest.
Arguments:
- dosage: bfloat16 [32768, 16384], P('samp', 'band'), may hold values from -1 to 2, as said below
Outputs:
- linkage: float32 [16384, 2048], P(('band', 'samp'))
The draws below stay inside these ranges and needn't reach their ends.
Inputs may be any that keep to these rules, and one draw needn't show every extreme that they name: -1 marks a missing call; every other entry is an imputed dosage between 0 and 2.
All inputs are finite; a program needn't handle non-finite values.
Results may differ from the reference program's by a relative error of at most 0.0015.
Values may be sent and summed in bfloat16 or wider, within the bound.
No kernel may reach another device: no remote copies, remote signals or barrier semaphores. Data moves between devices by JAX's collectives and lax.ppermute only.
A program may use at most 64 MiB of HBM per device.

```python
import jax
import jax.numpy as jnp
from jax import lax

TILE = 512
WIN = 2048
SAMPLES = 32768
SNPS = 16384


def draw_dosage(key, part):
    keys = jax.random.split(jax.random.fold_in(key, 17), 6)
    position = jnp.arange(SAMPLES, dtype=jnp.float32) / SAMPLES
    cohort = 0.5 + 1.5 * position
    freq = jax.random.uniform(keys[0], (SNPS,), jnp.float32, 0.05, 0.5)
    noise = 0.25 * jax.random.normal(keys[2], (SAMPLES, SNPS), jnp.float32)
    chance = jnp.clip(freq[None, :] * cohort[:, None], 0.0, 0.95)
    first = (jax.random.uniform(keys[1], (SAMPLES, SNPS), jnp.float32) < chance).astype(jnp.float32)
    second = (jax.random.uniform(keys[5], (SAMPLES, SNPS), jnp.float32) < chance).astype(jnp.float32)
    dose = jnp.clip(first + second + noise, 0.0, 2.0)
    rate = 0.02 + 0.1 * position
    missing = jax.random.uniform(keys[3], (SAMPLES, SNPS), jnp.float32) < rate[:, None]
    return jnp.where(missing, -1.0, dose).astype(jnp.bfloat16)


def setup_inputs(seed: int = 0) -> dict:
    key_of = jax.random.split(jax.random.key(seed), 2)
    return {
        "dosage": draw_dosage(jax.random.fold_in(key_of[1], 71), 0),
    }


def reference(dosage):
    raw = dosage.astype(jnp.float32)
    observed = (raw >= 0.0).astype(jnp.float32)
    values = observed * raw
    count = lax.optimization_barrier(jnp.sum(observed, axis=0))
    total = lax.optimization_barrier(jnp.sum(values, axis=0))
    square = lax.optimization_barrier(jnp.sum(values * values, axis=0))
    mean = (total + 1.0) / (count + 1.0)
    spread = (square - 2.0 * mean * total + count * mean * mean + 0.5) / (count + 1.0)
    scaled = (observed * (values - mean) * lax.rsqrt(spread)).astype(jnp.bfloat16)
    padded = jnp.pad(scaled, ((0, 0), (0, WIN - TILE)))

    def one_tile(index):
        rows = lax.dynamic_slice_in_dim(scaled, index * TILE, TILE, 1)
        columns = lax.dynamic_slice_in_dim(padded, index * TILE, WIN, 1)
        product = lax.dot_general(rows, columns, (((0,), (0,)), ((), ())), preferred_element_type=jnp.float32)
        return product / SAMPLES
    blocks = lax.map(one_tile, jnp.arange(SNPS // TILE, dtype=jnp.int32))
    return blocks.reshape(SNPS, WIN)
```

```python
import jax
import jax.numpy as jnp
from jax import lax
from jax.sharding import PartitionSpec as P

TILE = 512
WIN = 2048
AXES = ("band", "samp")
YS, XS, ZS, CORES = 8, 4, 8, 2


def index_of(y, x, z, core):
    return ((y * 2 + x // 2) * CORES + core) * (ZS * 2) + z * 2 + x % 2


def pairs_of(target_of):
    pairs = []
    for y in range(YS):
        for x in range(XS):
            for z in range(ZS):
                for core in range(CORES):
                    target = target_of(y, x, z, core)
                    if target is not None and target[0] >= 0:
                        pairs.append((index_of(y, x, z, core), index_of(*target)))
    return pairs


NEXT_CHIP = pairs_of(lambda y, x, z, c: (y, x - 2, z, c) if x >= 2 else (y - 1, x + 2, z, c))
EDGE = pairs_of(lambda y, x, z, c: (y, x, z, 0) if c == 1 else (y - 1, x, z, 1))
OTHER_CORE = pairs_of(lambda y, x, z, c: (y, x, z, 1 - c))
OTHER_HALF = pairs_of(lambda y, x, z, c: (y, x ^ 1, z, c))
Z_GROUPS = [[low + 2 * z for z in range(ZS)] for low in range(2)]


def sent(value, pairs):
    return lax.ppermute(value, AXES, pairs)


def over_z(value):
    return lax.all_to_all(value, "samp", 0, 0, tiled=True, axis_index_groups=Z_GROUPS)


def standardized(raw, stats):
    raw = raw.astype(jnp.float32)
    observed = (raw >= 0.0).astype(jnp.float32)
    return (observed * (observed * raw - stats[0]) * stats[1]).astype(jnp.bfloat16)


def on_device(dosage):
    half = TILE // 2
    samples = dosage.shape[0] * lax.axis_size("samp")
    core = lax.axis_index("band") % 2
    low = lax.axis_index("samp") % 2

    edge_raw = sent(dosage, EDGE)
    raw = dosage.astype(jnp.float32)
    observed = (raw >= 0.0).astype(jnp.float32)
    values = observed * raw
    sums = jnp.stack([observed.sum(0), values.sum(0), (values * values).sum(0)])
    sums = sums + sent(sums, OTHER_HALF)
    first, sums = lax.optimization_barrier((dosage[:, :half], sums))
    next_raw = sent(first, NEXT_CHIP)
    everyone = over_z(jnp.broadcast_to(sums[None], (ZS, *sums.shape)))
    count, total, square = everyone.sum(0)
    mean = (total + 1.0) / (count + 1.0)
    spread = (square - 2.0 * mean * total + count * mean * mean + 0.5) / (count + 1.0)
    stats = jnp.stack([mean, lax.rsqrt(spread)])
    next_stats = sent(stats[:, :half], NEXT_CHIP)
    edge_stats = sent(stats, EDGE)
    scaled = standardized(dosage, stats)
    next_second = sent(scaled[:, half:], NEXT_CHIP)

    def tile(panel):
        product = lax.dot_general(
            scaled, panel, (((0,), (0,)), ((), ())), preferred_element_type=jnp.float32
        )
        product = (product / samples).astype(jnp.bfloat16)
        arrived = over_z(product.reshape(ZS, -1, product.shape[1]))
        return arrived.astype(jnp.float32).sum(0)

    def owned(rows):
        count = rows.shape[0] // 2
        mine = lax.dynamic_slice_in_dim(rows, low * count, count, 0)
        other = lax.dynamic_slice_in_dim(rows, (1 - low) * count, count, 0)
        return mine + sent(other, OTHER_HALF)

    own = tile(scaled)
    edge = tile(standardized(edge_raw, edge_stats))
    next_first = standardized(next_raw, next_stats)
    swapped_first = sent(next_first, OTHER_CORE)
    firsts = tile(jnp.concatenate([next_first, swapped_first], axis=1))
    swapped_second = sent(next_second, OTHER_CORE)
    seconds = tile(jnp.concatenate([next_second, swapped_second], axis=1))
    early = owned(jnp.concatenate([own, edge], axis=1))
    firsts = owned(firsts)
    seconds = owned(seconds)
    own, edge = early[:, :TILE], early[:, TILE:]
    nexts = jnp.concatenate([firsts[:, :half], seconds[:, :half]], axis=1)
    swaps = jnp.concatenate([firsts[:, half:], seconds[:, half:]], axis=1)
    even = core == 0
    return jnp.concatenate(
        [own, jnp.where(even, edge, swaps), nexts, jnp.where(even, swaps, edge)], axis=1
    )


def solution(mesh):
    return jax.shard_map(
        on_device,
        mesh=mesh,
        in_specs=(P("samp", "band"),),
        out_specs=P(("band", "samp"), None),
        check_vma=False,
    )
```

```python
import jax
import jax.numpy as jnp
from jax import lax
from jax.sharding import PartitionSpec as P


TILE = 512
AXES = ("band", "samp")
YS, XS, ZS, CORES = 8, 4, 8, 2


def index_of(y, x, z, core):
    return ((y * 2 + x // 2) * CORES + core) * (ZS * 2) + z * 2 + x % 2


def pairs_of(target_of):
    pairs = []
    for y in range(YS):
        for x in range(XS):
            for z in range(ZS):
                for core in range(CORES):
                    target = target_of(y, x, z, core)
                    if target is not None and target[0] >= 0:
                        pairs.append((index_of(y, x, z, core), index_of(*target)))
    return pairs


NEXT_CHIP = pairs_of(lambda y, x, z, c: (y, x - 2, z, c) if x >= 2 else (y - 1, x + 2, z, c))
EDGE = pairs_of(lambda y, x, z, c: (y, x, z, 0) if c == 1 else (y - 1, x, z, 1))
OTHER_CORE = pairs_of(lambda y, x, z, c: (y, x, z, 1 - c))
OTHER_HALF = pairs_of(lambda y, x, z, c: (y, x ^ 1, z, c))
Z_GROUPS = [[low + 2 * z for z in range(ZS)] for low in range(2)]


def sent(value, pairs):
    return lax.ppermute(value, AXES, pairs)


def over_z(value):
    return lax.all_to_all(value, "samp", 0, 0, tiled=True, axis_index_groups=Z_GROUPS)


def over_samp(value):
    return lax.all_to_all(value, "samp", 0, 0, tiled=True)


def standardized(raw, stats):
    raw = raw.astype(jnp.float32)
    observed = (raw >= 0.0).astype(jnp.float32)
    return (observed * (observed * raw - stats[0]) * stats[1]).astype(jnp.bfloat16)


def assemble(even, own, edge, first_next, first_swap, last):
    half = first_next.shape[1]
    last = last.astype(jnp.float32).sum(0)
    nexts = jnp.concatenate([first_next, last[:, :half]], axis=1)
    swaps = jnp.concatenate([first_swap, last[:, half:]], axis=1)
    return jnp.concatenate(
        [own, jnp.where(even, edge, swaps), nexts, jnp.where(even, swaps, edge)], axis=1
    )


def on_device(dosage):
    half = TILE // 2
    samples = dosage.shape[0] * lax.axis_size("samp")
    even = lax.axis_index("band") % 2 == 0
    low = lax.axis_index("samp") % 2

    edge_raw = sent(dosage, EDGE)
    raw = dosage.astype(jnp.float32)
    observed = (raw >= 0.0).astype(jnp.float32)
    values = observed * raw
    sums = jnp.stack([observed.sum(0), values.sum(0), (values * values).sum(0)])
    everyone = over_samp(jnp.broadcast_to(sums[None], (2 * ZS, *sums.shape)))
    count, total, square = everyone.sum(0)
    mean = (total + 1.0) / (count + 1.0)
    spread = (square - 2.0 * mean * total + count * mean * mean + 0.5) / (count + 1.0)
    stats = jnp.stack([mean, lax.rsqrt(spread)])
    scaled = standardized(dosage, stats)
    next_a = sent(scaled[:, :half], NEXT_CHIP)
    edge_stats = sent(stats, EDGE)
    next_b = sent(scaled[:, half:], NEXT_CHIP)

    def tile(panel):
        product = lax.dot_general(
            scaled, panel, (((0,), (0,)), ((), ())), preferred_element_type=jnp.float32
        )
        return (product / samples).astype(jnp.bfloat16)

    own = tile(scaled)
    edge = tile(standardized(edge_raw, edge_stats))
    early = jnp.concatenate([own, edge], axis=1)
    early = over_z(early.reshape(ZS, -1, 2 * TILE)).astype(jnp.float32).sum(0)
    swap_a = sent(next_a, OTHER_CORE)
    mid = tile(jnp.concatenate([next_a, swap_a], axis=1))
    mid = over_samp(mid.reshape(2 * ZS, -1, TILE)).astype(jnp.float32).sum(0)
    count = early.shape[0] // 2
    mine = lax.dynamic_slice_in_dim(early, low * count, count, 0)
    other = lax.dynamic_slice_in_dim(early, (1 - low) * count, count, 0)
    early = mine + sent(other, OTHER_HALF)
    swap_b = sent(next_b, OTHER_CORE)
    last = tile(jnp.concatenate([next_b, swap_b], axis=1))
    last = over_samp(last.reshape(2 * ZS, -1, TILE))
    return assemble(even, early[:, :TILE], early[:, TILE:], mid[:, :half], mid[:, half:], last)


def solution(mesh):
    return jax.shard_map(
        on_device,
        mesh=mesh,
        in_specs=(P("samp", "band"),),
        out_specs=P(("band", "samp"), None),
        check_vma=False,
    )
```

```python
import jax
import jax.numpy as jnp
from jax import lax
from jax.experimental.layout import Layout, with_layout_constraint
from jax.sharding import PartitionSpec as P


TILE = 512
AXES = ("band", "samp")
YS, XS, ZS, CORES = 8, 4, 8, 2


def index_of(y, x, z, core):
    return ((y * 2 + x // 2) * CORES + core) * (ZS * 2) + z * 2 + x % 2


def pairs_of(target_of):
    pairs = []
    for y in range(YS):
        for x in range(XS):
            for z in range(ZS):
                for core in range(CORES):
                    target = target_of(y, x, z, core)
                    if target is not None and target[0] >= 0:
                        pairs.append((index_of(y, x, z, core), index_of(*target)))
    return pairs


NEXT_CHIP = pairs_of(lambda y, x, z, c: (y, x - 2, z, c) if x >= 2 else (y - 1, x + 2, z, c))
EDGE = pairs_of(lambda y, x, z, c: (y, x, z, 0) if c == 1 else (y - 1, x, z, 1))
OTHER_CORE = pairs_of(lambda y, x, z, c: (y, x, z, 1 - c))
OTHER_HALF = pairs_of(lambda y, x, z, c: (y, x ^ 1, z, c))
Z_GROUPS = [[low + 2 * z for z in range(ZS)] for low in range(2)]


def sent(value, pairs):
    return lax.ppermute(value, AXES, pairs)


def over_z(value):
    return lax.all_to_all(value, "samp", 0, 0, tiled=True, axis_index_groups=Z_GROUPS)


def over_samp(value):
    return lax.all_to_all(value, "samp", 0, 0, tiled=True)


def standardized(raw, stats):
    raw = raw.astype(jnp.float32)
    observed = (raw >= 0.0).astype(jnp.float32)
    return (observed * (observed * raw - stats[0]) * stats[1]).astype(jnp.bfloat16)


def assembled(even, early, mid, last):
    half = mid.shape[1] // 2
    own, edge = early[:, :TILE], early[:, TILE:]
    low, high, next_low, next_high = mid[:, half:], last[:, half:], mid[:, :half], last[:, :half]
    edge_low, edge_high = edge[:, :half], edge[:, half:]
    return jnp.concatenate(
        [
            own,
            jnp.where(even, edge_low, low),
            jnp.where(even, edge_high, high),
            next_low,
            next_high,
            jnp.where(even, low, edge_low),
            jnp.where(even, high, edge_high),
        ],
        axis=1,
    )


def on_device(dosage):
    half = TILE // 2
    samples = dosage.shape[0] * lax.axis_size("samp")
    even = lax.axis_index("band") % 2 == 0
    low = lax.axis_index("samp") % 2

    edge_raw = sent(dosage, EDGE)
    raw = dosage.astype(jnp.float32)
    observed = (raw >= 0.0).astype(jnp.float32)
    values = observed * raw
    sums = jnp.stack([observed.sum(0), values.sum(0), (values * values).sum(0)])
    everyone = over_samp(jnp.broadcast_to(sums[None], (2 * ZS, *sums.shape)))
    count, total, square = everyone.sum(0)
    mean = (total + 1.0) / (count + 1.0)
    spread = (square - 2.0 * mean * total + count * mean * mean + 0.5) / (count + 1.0)
    stats = jnp.stack([mean, lax.rsqrt(spread)])
    edge_stats = sent(stats, EDGE)
    next_a = sent(standardized(dosage[:, :half], stats[:, :half]), NEXT_CHIP)
    scaled = standardized(dosage, stats)
    scaled = lax.optimization_barrier(scaled)
    next_b = sent(scaled[:, half:], NEXT_CHIP)

    def tile(panel):
        product = lax.dot_general(
            scaled, panel, (((0,), (0,)), ((), ())), preferred_element_type=jnp.float32
        )
        product = (product / samples).astype(jnp.bfloat16)
        return with_layout_constraint(product, Layout(major_to_minor=(0, 1)))

    own = tile(scaled)
    edge = tile(standardized(edge_raw, edge_stats))
    early = jnp.concatenate([own, edge], axis=1)
    early = over_z(early.reshape(ZS, -1, 2 * TILE)).astype(jnp.float32).sum(0)
    swap_a = sent(next_a, OTHER_CORE)
    mid = tile(jnp.concatenate([next_a, swap_a], axis=1))
    mid = over_z(mid.reshape(ZS, -1, TILE)).astype(jnp.float32).sum(0)
    count = early.shape[0] // 2

    def pair_sum(rows):
        mine = lax.dynamic_slice_in_dim(rows, low * count, count, 0)
        other = lax.dynamic_slice_in_dim(rows, (1 - low) * count, count, 0)
        return mine + sent(other, OTHER_HALF)

    swap_b = sent(next_b, OTHER_CORE)
    last = tile(jnp.concatenate([next_b, swap_b], axis=1))
    last = over_samp(last.reshape(2 * ZS, -1, TILE))
    early = pair_sum(early)
    mid = pair_sum(mid)
    return assembled(even, early, mid, last.astype(jnp.float32).sum(0))


def solution(mesh):
    return jax.shard_map(
        on_device,
        mesh=mesh,
        in_specs=(P("samp", "band"),),
        out_specs=P(("band", "samp"), None),
        check_vma=False,
    )
```

```python
import jax
import jax.numpy as jnp
from jax import lax
from jax.experimental.layout import Layout, with_layout_constraint
from jax.sharding import PartitionSpec as P


TILE = 512
WIN = 2048
AXES = ("band", "samp")
YS, XS, ZS, CORES = 8, 4, 8, 2


def index_of(y, x, z, core):
    return ((y * 2 + x // 2) * CORES + core) * (ZS * 2) + z * 2 + x % 2


def pairs_of(target_of):
    pairs = []
    for y in range(YS):
        for x in range(XS):
            for z in range(ZS):
                for core in range(CORES):
                    target = target_of(y, x, z, core)
                    if target is not None and target[0] >= 0:
                        pairs.append((index_of(y, x, z, core), index_of(*target)))
    return pairs


NEXT_CHIP = pairs_of(lambda y, x, z, c: (y, x - 2, z, c) if x >= 2 else (y - 1, x + 2, z, c))
EDGE = pairs_of(lambda y, x, z, c: (y, x, z, 0) if c == 1 else (y - 1, x, z, 1))
OTHER_CORE = pairs_of(lambda y, x, z, c: (y, x, z, 1 - c))
OTHER_HALF = pairs_of(lambda y, x, z, c: (y, x ^ 1, z, c))
Z_GROUPS = [[low + 2 * z for z in range(ZS)] for low in range(2)]


def sent(value, pairs):
    return lax.ppermute(value, AXES, pairs)


def over_z(value):
    return lax.all_to_all(value, "samp", 0, 0, tiled=True, axis_index_groups=Z_GROUPS)


def over_samp(value):
    return lax.all_to_all(value, "samp", 0, 0, tiled=True)


def standardized(raw, stats):
    raw = raw.astype(jnp.float32)
    observed = (raw >= 0.0).astype(jnp.float32)
    return (observed * (observed * raw - stats[0]) * stats[1]).astype(jnp.bfloat16)


def assembled(even, early, mid, last):
    half = mid.shape[1] // 2
    own, edge, low = early[:, :TILE], early[:, TILE:], mid[:, half:]
    high, none = edge[:, half:], jnp.zeros_like(low)
    swapped_at_3 = [jnp.where(even, edge[:, :half], low), jnp.where(even, high, none)]
    swapped_at_1 = [jnp.where(even, low, edge[:, :half]), jnp.where(even, none, high)]
    base = jnp.concatenate([own, *swapped_at_3, mid[:, :half], none, *swapped_at_1], axis=1)
    base, last = lax.optimization_barrier((base, last))

    def placed(value, start):
        return jnp.pad(value, ((0, 0), (start, WIN - start - value.shape[1])))

    at_1, at_3 = (placed(last[:, half:], t * TILE + half) for t in (1, 3))
    return base + placed(last[:, :half], 2 * TILE + half) + jnp.where(even, at_3, at_1)


def widened(value, width):
    return lax.optimization_barrier(jnp.pad(value, ((0, 0), (0, width))))


def filled(wide, value):
    start = wide.shape[1] - value.shape[1]
    return lax.optimization_barrier(lax.dynamic_update_slice(wide, value, (0, start)))


def on_device(dosage):
    half = TILE // 2
    samples = dosage.shape[0] * lax.axis_size("samp")
    even = lax.axis_index("band") % 2 == 0
    low = lax.axis_index("samp") % 2

    edge_raw = sent(dosage, EDGE)
    raw = dosage.astype(jnp.float32)
    observed = (raw >= 0.0).astype(jnp.float32)
    values = observed * raw
    sums = jnp.stack([observed.sum(0), values.sum(0), (values * values).sum(0)])
    everyone = over_samp(jnp.broadcast_to(sums[None], (2 * ZS, *sums.shape)))
    count, total, square = everyone.sum(0)
    mean = (total + 1.0) / (count + 1.0)
    spread = (square - 2.0 * mean * total + count * mean * mean + 0.5) / (count + 1.0)
    stats = jnp.stack([mean, lax.rsqrt(spread)])
    edge_stats = sent(stats, EDGE)
    next_a = sent(standardized(dosage[:, :half], stats[:, :half]), NEXT_CHIP)
    scaled = standardized(dosage, stats)
    scaled = lax.optimization_barrier(scaled)
    next_b = sent(scaled[:, half:], NEXT_CHIP)

    def tile(panel):
        product = lax.dot_general(
            scaled, panel, (((0,), (0,)), ((), ())), preferred_element_type=jnp.float32
        )
        product = (product / samples).astype(jnp.bfloat16)
        return with_layout_constraint(product, Layout(major_to_minor=(0, 1)))

    own = tile(scaled)
    edge = tile(standardized(edge_raw, edge_stats))
    early = jnp.concatenate([own, edge], axis=1)
    early = over_z(early.reshape(ZS, -1, 2 * TILE)).astype(jnp.float32).sum(0)
    swap_a = sent(next_a, OTHER_CORE)
    mid = tile(filled(widened(next_a, half), swap_a))
    mid = over_z(mid.reshape(ZS, -1, TILE)).astype(jnp.float32).sum(0)
    count = early.shape[0] // 2

    def pair_sum(rows):
        mine = lax.dynamic_slice_in_dim(rows, low * count, count, 0)
        other = lax.dynamic_slice_in_dim(rows, (1 - low) * count, count, 0)
        return mine + sent(other, OTHER_HALF)

    swap_b = sent(next_b, OTHER_CORE)
    last = tile(filled(widened(next_b, half), swap_b))
    last = over_samp(last.reshape(2 * ZS, -1, TILE))
    early = pair_sum(early)
    mid = pair_sum(mid)
    return assembled(even, early, mid, last.astype(jnp.float32).sum(0))


def solution(mesh):
    return jax.shard_map(
        on_device,
        mesh=mesh,
        in_specs=(P("samp", "band"),),
        out_specs=P(("band", "samp"), None),
        check_vma=False,
    )
```

```python
import jax
import jax.numpy as jnp
from jax import lax
from jax.experimental.layout import Layout, with_layout_constraint
from jax.sharding import PartitionSpec as P


TILE = 512
WIN = 2048
EDGE_FIRST = 384
AXES = ("band", "samp")
YS, XS, ZS, CORES = 8, 4, 8, 2


def index_of(y, x, z, core):
    return ((y * 2 + x // 2) * CORES + core) * (ZS * 2) + z * 2 + x % 2


def pairs_of(target_of):
    pairs = []
    for y in range(YS):
        for x in range(XS):
            for z in range(ZS):
                for core in range(CORES):
                    target = target_of(y, x, z, core)
                    if target is not None and target[0] >= 0:
                        pairs.append((index_of(y, x, z, core), index_of(*target)))
    return pairs


NEXT_CHIP = pairs_of(lambda y, x, z, c: (y, x - 2, z, c) if x >= 2 else (y - 1, x + 2, z, c))
EDGE = pairs_of(lambda y, x, z, c: (y, x, z, 0) if c == 1 else (y - 1, x, z, 1))
OTHER_CORE = pairs_of(lambda y, x, z, c: (y, x, z, 1 - c))
OTHER_HALF = pairs_of(lambda y, x, z, c: (y, x ^ 1, z, c))
Z_GROUPS = [[low + 2 * z for z in range(ZS)] for low in range(2)]


def sent(value, pairs):
    return lax.ppermute(value, AXES, pairs)


def over_z(value):
    return lax.all_to_all(value, "samp", 0, 0, tiled=True, axis_index_groups=Z_GROUPS)


def over_samp(value):
    return lax.all_to_all(value, "samp", 0, 0, tiled=True)


def standardized(raw, stats):
    raw = raw.astype(jnp.float32)
    observed = (raw >= 0.0).astype(jnp.float32)
    return (observed * (observed * raw - stats[0]) * stats[1]).astype(jnp.bfloat16)


def assembled(even, early, mid, last):
    half = mid.shape[1] // 2
    own, edge, low = early[:, :TILE], early[:, TILE:], mid[:, half:]
    high, none = edge[:, half:], jnp.zeros_like(low)
    swapped_at_3 = [jnp.where(even, edge[:, :half], low), jnp.where(even, high, none)]
    swapped_at_1 = [jnp.where(even, low, edge[:, :half]), jnp.where(even, none, high)]
    base = jnp.concatenate([own, *swapped_at_3, mid[:, :half], none, *swapped_at_1], axis=1)
    base, last = lax.optimization_barrier((base, last))

    def placed(value, start):
        return jnp.pad(value, ((0, 0), (start, WIN - start - value.shape[1])))

    at_1, at_3 = (placed(last[:, half:], t * TILE + half) for t in (1, 3))
    return base + placed(last[:, :half], 2 * TILE + half) + jnp.where(even, at_3, at_1)


def widened(value, width):
    return lax.optimization_barrier(jnp.pad(value, ((0, 0), (0, width))))


def filled(wide, value):
    start = wide.shape[1] - value.shape[1]
    return lax.optimization_barrier(lax.dynamic_update_slice(wide, value, (0, start)))


def on_device(dosage):
    half = TILE // 2
    samples = dosage.shape[0] * lax.axis_size("samp")
    even = lax.axis_index("band") % 2 == 0
    low = lax.axis_index("samp") % 2

    edge_raw = sent(dosage, EDGE)
    raw = dosage.astype(jnp.float32)
    observed = (raw >= 0.0).astype(jnp.float32)
    values = observed * raw
    sums = jnp.stack([observed.sum(0), values.sum(0), (values * values).sum(0)])
    everyone = over_samp(jnp.broadcast_to(sums[None], (2 * ZS, *sums.shape)))
    count, total, square = everyone.sum(0)
    mean = (total + 1.0) / (count + 1.0)
    spread = (square - 2.0 * mean * total + count * mean * mean + 0.5) / (count + 1.0)
    stats = jnp.stack([mean, lax.rsqrt(spread)])
    edge_stats = sent(stats, EDGE)
    next_a = sent(standardized(dosage[:, :half], stats[:, :half]), NEXT_CHIP)
    scaled = standardized(dosage, stats)
    scaled = lax.optimization_barrier(scaled)
    next_b = sent(scaled[:, half:], NEXT_CHIP)

    def tile(panel):
        product = lax.dot_general(
            scaled, panel, (((0,), (0,)), ((), ())), preferred_element_type=jnp.float32
        )
        product = (product / samples).astype(jnp.bfloat16)
        return with_layout_constraint(product, Layout(major_to_minor=(0, 1)))

    own = tile(scaled)
    edge_rest = lax.optimization_barrier(
        standardized(edge_raw[:, EDGE_FIRST:], edge_stats[:, EDGE_FIRST:])
    )
    edge = tile(standardized(edge_raw[:, :EDGE_FIRST], edge_stats[:, :EDGE_FIRST]))
    early = jnp.concatenate([own, edge], axis=1)
    early = over_z(early.reshape(ZS, -1, TILE + EDGE_FIRST)).astype(jnp.float32).sum(0)
    swap_a = sent(next_a, OTHER_CORE)
    mid = tile(filled(widened(jnp.concatenate([next_a, edge_rest], axis=1), half), swap_a))
    mid = over_z(mid.reshape(ZS, -1, mid.shape[1])).astype(jnp.float32).sum(0)
    count = early.shape[0] // 2

    def pair_sum(rows):
        mine = lax.dynamic_slice_in_dim(rows, low * count, count, 0)
        other = lax.dynamic_slice_in_dim(rows, (1 - low) * count, count, 0)
        return mine + sent(other, OTHER_HALF)

    swap_b = sent(next_b, OTHER_CORE)
    last = tile(filled(widened(next_b, half), swap_b))
    last = over_samp(last.reshape(2 * ZS, -1, TILE))
    early = pair_sum(early)
    mid = pair_sum(mid)
    rest_at = half + TILE - EDGE_FIRST
    early = jnp.concatenate([early, mid[:, half:rest_at]], axis=1)
    mid = jnp.concatenate([mid[:, :half], mid[:, rest_at:]], axis=1)
    return assembled(even, early, mid, last.astype(jnp.float32).sum(0))


def solution(mesh):
    return jax.shard_map(
        on_device,
        mesh=mesh,
        in_specs=(P("samp", "band"),),
        out_specs=P(("band", "samp"), None),
        check_vma=False,
    )
```
